32 devices in a mesh: cfg: 2 (over x), space: 8 (over z, y), tm: 2 (over core).
Axes of the slice: x: 2, y: 2, z: 4, core: 2. Of those that a mesh axis runs over, the one named last changes fastest.
Arguments:
- vectors: bfloat16 [4, 64, 6, 8192], P(('cfg', 'tm'), 'space'), parts along dimension 0, may hold values from -0.5 to 0.5
- gauge_links: bfloat16 [4, 3, 18, 8192], P(('cfg', 'tm'), None, None, 'space'), parts along dimension 0, may hold values from -3 to 3
- momenta: int32 [8, 3], replicated, may hold values from -2 to 2
- directions: int32 [3], replicated, may hold values from 0 to 2, each once
Outputs:
- elementals: float32 [64, 4, 8, 3, 128], P('space', ('cfg', 'tm')), parts along dimension 1
The draws below stay inside these ranges and needn't reach their ends.
There are 2 independent parts, one for each index of `cfg`. The reference program is written for one: setup_inputs(seed, part) draws one part's arguments, and reference() takes and returns one part's arrays. A program takes and returns all parts, laid end to end along the dimension named above; an argument that names none is the same for every part. Nothing has to cross between parts.
Inputs may be any that keep to these rules, and one draw needn't show every extreme that they name: `momenta`: integer momentum components, in units of 2 pi over the lattice extent. Each of the directions 0, 1, 2 appears once.
All inputs are finite; a program needn't handle non-finite values.
Results may differ from the reference program's by a relative error of at most 0.005.
Values may be sent and summed in bfloat16 or wider, within the bound.
A program may use at most 128 MiB of HBM per device.

```python
import math
import jax
import jax.numpy as jnp
from jax import lax

NEV = 64
LXY = 32
NMOM = 8
NDIR = 3
LZ = 8
SITES = 8192
T_SIZE = 2


def place_ends(drawn, key, least, high):
    longest = drawn.shape.index(max(drawn.shape))
    spots = []
    for shift in (0, 1):
        where = [jax.random.randint(jax.random.fold_in(key, axis), (), 0, length) for axis, length in enumerate(drawn.shape)]
        where[longest] = (where[longest] + shift) % drawn.shape[longest]
        spots.append(tuple(where))
    return drawn.at[spots[0]].set(least).at[spots[1]].set(high)


def with_spikes(values, stream_key, source, target, blocks, factor):
    owner, partner = [(jnp.arange(values.shape[position]) // (values.shape[position] // blocks)).reshape([-1 if axis == position else 1 for axis in range(values.ndim)]) for position in (source, target)]
    chosen = jax.random.permutation(stream_key, blocks)[partner]
    strong = (owner == chosen) | (owner == (partner + blocks // 2) % blocks)
    return jnp.where(strong, factor * values, values)


def level_of(key, extent, shards, smallest, top_value):
    factor_of, own = 1.0, jax.random.fold_in(key, 6)
    for axis_at, shards_of in shards:
        heights = jnp.exp(jax.random.uniform(jax.random.fold_in(own, axis_at), (shards_of,), jnp.float32, smallest / len(shards), top_value / len(shards)))
        factor_of = factor_of * jnp.repeat(heights, extent[axis_at] // shards_of).reshape([-1 if axis == axis_at else 1 for axis in range(len(extent))])
    return factor_of


def centred(rng, dims, scale, most, split=(), kind=jnp.bfloat16):
    level = level_of(rng, dims, split, -0.22, 0.18) if split else 1.0
    entries = jax.random.normal(rng, dims, jnp.float32) * scale * level
    return jnp.minimum(jnp.maximum(entries, -most), most).astype(kind)


def noise_with(own_key, extent, spread, most, cuts, heavy, kind=jnp.bfloat16):
    values = spread * jax.random.normal(own_key, extent, jnp.float32)
    if cuts:
        values = values * level_of(own_key, extent, cuts, -0.22, 0.18)
    return jnp.clip(with_spikes(values, jax.random.fold_in(own_key, 3), *heavy), -most, most).astype(kind)


def setup_inputs(seed: int = 0, part: int = 0) -> dict:
    arg_keys = jax.random.split(jax.random.key(seed), 5)
    part_keys = jax.random.split(jax.random.fold_in(arg_keys[4], part), 5)
    vectors = noise_with(part_keys[0], (T_SIZE, NEV, 6, SITES), ((6 * SITES) ** -0.25), 0.5, ((0, 2), (1, 8)), (3, 1, 8, 2.0))
    gauge_links = centred(part_keys[1], (T_SIZE, 3, 18, SITES), 0.5, 3.0, ((0, 2), (3, 8)))
    momenta = place_ends(jax.random.randint(arg_keys[2], (NMOM, 3), -2, 3), jax.random.fold_in(arg_keys[2], 1), -2, 2).astype(jnp.int32)
    directions = jax.random.permutation(arg_keys[3], 3).astype(jnp.int32)
    return dict(vectors=vectors, gauge_links=gauge_links, momenta=momenta, directions=directions)


TWO_PI = 2.0 * math.pi


def apply_link(link, field_f32):
    real_rows = []
    imag_rows = []
    for row_a in range(3):
        link_re = link[0, row_a, 0][None]
        link_im = link[1, row_a, 0][None]
        real_acc = link_re * field_f32[:, 0, 0] - link_im * field_f32[:, 1, 0]
        imag_acc = link_re * field_f32[:, 1, 0] + link_im * field_f32[:, 0, 0]
        for col_b in range(1, 3):
            link_re = link[0, row_a, col_b][None]
            link_im = link[1, row_a, col_b][None]
            real_acc = real_acc + link_re * field_f32[:, 0, col_b] - link_im * field_f32[:, 1, col_b]
            imag_acc = imag_acc + link_re * field_f32[:, 1, col_b] + link_im * field_f32[:, 0, col_b]
        real_rows.append(real_acc)
        imag_rows.append(imag_acc)
    return jnp.stack([jnp.stack(real_rows, axis=1), jnp.stack(imag_rows, axis=1)], axis=1)


def adjoint(link):
    return jnp.stack([jnp.swapaxes(link[0], 0, 1), -jnp.swapaxes(link[1], 0, 1)])


def pack_terms(derivative, eig_count):
    rounded = derivative.astype(jnp.bfloat16)
    rounded_re = rounded[:, 0]
    rounded_im = rounded[:, 1]
    swapped = jnp.stack([rounded_im, -rounded_re], axis=1)
    return jnp.concatenate([rounded, swapped], axis=0).reshape(2 * eig_count, -1)


def phase_angles(momenta, z_offset, depth_planes, z_length):
    z_coord = (z_offset + jnp.arange(depth_planes, dtype=jnp.int32)).astype(jnp.int32)
    y_coord = jnp.arange(LXY, dtype=jnp.int32)
    x_coord = jnp.arange(LXY, dtype=jnp.int32)
    mom_x = momenta[:, 0][:, None, None, None]
    mom_y = momenta[:, 1][:, None, None, None]
    mom_z = momenta[:, 2][:, None, None, None]
    fraction = ((mom_x * x_coord[None, None, None, :]) % LXY).astype(jnp.float32) / LXY
    fraction = fraction + ((mom_y * y_coord[None, None, :, None]) % LXY).astype(jnp.float32) / LXY
    fraction = fraction + ((mom_z * z_coord[None, :, None, None]) % z_length).astype(jnp.float32) / z_length
    return TWO_PI * fraction


def phase_twist(row_block, cosine_table, sine_table):
    vec_re = row_block[:, 0][None]
    vec_im = row_block[:, 1][None]
    cos_b = cosine_table[:, None, None]
    sin_b = sine_table[:, None, None]
    real_part = vec_re * cos_b - vec_im * sin_b
    imag_part = vec_re * sin_b + vec_im * cos_b
    twisted = jnp.stack([real_part, imag_part], axis=2).astype(jnp.bfloat16)
    return twisted.reshape(cosine_table.shape[0] * row_block.shape[0], -1)


def reference(vectors, gauge_links, momenta, directions):
    slab_count = vectors.shape[0]
    eig_count = vectors.shape[1]
    angles = phase_angles(momenta, 0, LZ, LZ)
    cosine_all = jnp.cos(angles)
    sine_all = jnp.sin(angles)
    per_slab = []
    for slab in range(slab_count):
        field_f32 = vectors[slab].reshape(eig_count, 2, 3, LZ, LXY, LXY).astype(jnp.float32)
        slab_links = gauge_links[slab].reshape(3, 2, 3, 3, LZ, LXY, LXY).astype(jnp.float32)
        packed_list = []
        for dir_index, roll_axis in ((0, -1), (1, -2), (2, -3)):
            forward = apply_link(slab_links[dir_index], jnp.roll(field_f32, -1, axis=roll_axis))
            backward = jnp.roll(apply_link(adjoint(slab_links[dir_index]), field_f32), 1, axis=roll_axis)
            packed_list.append(pack_terms(0.5 * (forward - backward), eig_count))
        packed_all = jnp.stack(packed_list)
        per_mom = []
        for mom_index in range(NMOM):
            twisted = phase_twist(field_f32, cosine_all[mom_index:mom_index + 1], sine_all[mom_index:mom_index + 1]).astype(jnp.float32)
            per_dir = []
            for dir_slot in range(NDIR):
                chosen = packed_all[directions[dir_slot]].astype(jnp.float32)
                per_dir.append(jnp.dot(twisted, chosen.T, precision=lax.Precision.HIGHEST))
            per_mom.append(jnp.stack(per_dir, axis=1))
        per_slab.append(jnp.stack(per_mom, axis=1))
    return jnp.stack(per_slab, axis=1)
```

```python
import math

import jax
import jax.numpy as jnp
from jax import lax
from jax.experimental import pallas as pl
from jax.experimental.pallas import tpu as pltpu
from jax.sharding import PartitionSpec as P

LXY = 32
NMOM = 8
NDIR = 3


TWO_PI = 2.0 * math.pi


def with_halo(cells, sides, width):
    for axis, dim in sides:
        count = lax.axis_size(axis)
        head = lax.slice_in_dim(cells, 0, width, axis=dim)
        tail = lax.slice_in_dim(cells, cells.shape[dim] - width, cells.shape[dim], axis=dim)
        cells = jnp.concatenate(
            [
                lax.ppermute(tail, axis, [(i, (i + 1) % count) for i in range(count)]),
                cells,
                lax.ppermute(head, axis, [((i + 1) % count, i) for i in range(count)]),
            ],
            axis=dim,
        )
    return cells


def from_behind(block, axis, distance):
    devices = range(lax.axis_size(axis))
    route = [((i - distance) % len(devices), i) for i in devices]
    return lax.ppermute(block, axis, route)


def apply_link(link, field_f32):
    real_rows = []
    imag_rows = []
    for row_a in range(3):
        link_re = link[0, row_a, 0][None]
        link_im = link[1, row_a, 0][None]
        real_acc = link_re * field_f32[:, 0, 0] - link_im * field_f32[:, 1, 0]
        imag_acc = link_re * field_f32[:, 1, 0] + link_im * field_f32[:, 0, 0]
        for col_b in range(1, 3):
            link_re = link[0, row_a, col_b][None]
            link_im = link[1, row_a, col_b][None]
            real_acc = (
                real_acc + link_re * field_f32[:, 0, col_b] - link_im * field_f32[:, 1, col_b]
            )
            imag_acc = (
                imag_acc + link_re * field_f32[:, 1, col_b] + link_im * field_f32[:, 0, col_b]
            )
        real_rows.append(real_acc)
        imag_rows.append(imag_acc)
    return jnp.stack([jnp.stack(real_rows, axis=1), jnp.stack(imag_rows, axis=1)], axis=1)


def adjoint(link):
    return jnp.stack([jnp.swapaxes(link[0], 0, 1), -jnp.swapaxes(link[1], 0, 1)])


def pack_terms(derivative, eig_count):
    rounded = derivative.astype(jnp.bfloat16)
    rounded_re = rounded[:, 0]
    rounded_im = rounded[:, 1]
    swapped = jnp.stack([rounded_im, -rounded_re], axis=1)
    return jnp.concatenate([rounded, swapped], axis=0).reshape(2 * eig_count, -1)


def phase_angles(momenta, z_offset, depth_planes, z_length):
    z_coord = z_offset + jnp.arange(depth_planes, dtype=jnp.int32)
    y_coord = jnp.arange(LXY, dtype=jnp.int32)
    x_coord = jnp.arange(LXY, dtype=jnp.int32)
    mom_x = momenta[:, 0][:, None, None, None]
    mom_y = momenta[:, 1][:, None, None, None]
    mom_z = momenta[:, 2][:, None, None, None]
    fraction = (mom_x * x_coord[None, None, None, :] % LXY).astype(jnp.float32) / LXY
    fraction = fraction + (mom_y * y_coord[None, None, :, None] % LXY).astype(jnp.float32) / LXY
    fraction = (
        fraction + (mom_z * z_coord[None, :, None, None] % z_length).astype(jnp.float32) / z_length
    )
    return TWO_PI * fraction


def phase_twist(row_block, cosine_table, sine_table):
    vec_re = row_block[:, 0][None]
    vec_im = row_block[:, 1][None]
    cos_b = cosine_table[:, None, None]
    sin_b = sine_table[:, None, None]
    real_part = vec_re * cos_b - vec_im * sin_b
    imag_part = vec_re * sin_b + vec_im * cos_b
    twisted = jnp.stack([real_part, imag_part], axis=2).astype(jnp.bfloat16)
    return twisted.reshape(cosine_table.shape[0] * row_block.shape[0], -1)


def shards_by_plane(vectors, gauge_links, momenta, directions):
    space_count = lax.axis_size("space")
    slab_count = vectors.shape[0]
    eig_local = vectors.shape[1]
    eig_count = eig_local * space_count
    plane_size = LXY * LXY
    depth_planes = gauge_links.shape[3] // plane_size
    blocks = vectors.reshape(slab_count, eig_local, 6, space_count, depth_planes, plane_size)
    regrouped = lax.all_to_all(blocks, "space", split_axis=3, concat_axis=1, tiled=True)
    local_block = regrouped.reshape(slab_count, eig_count, 6, depth_planes, plane_size)
    extended = with_halo(local_block, (("space", 3),), 1)
    z_links = gauge_links[:, 2].reshape(slab_count, 18, depth_planes, plane_size)
    link_below = from_behind(z_links[:, :, depth_planes - 1, :], "space", 1)
    links_below = jnp.concatenate(
        [link_below[:, :, None, :], z_links[:, :, : depth_planes - 1, :]], axis=2
    )
    z_offset = lax.axis_index("space") * depth_planes
    angles = phase_angles(momenta, z_offset, depth_planes, depth_planes * space_count)
    cosine_all = jnp.cos(angles)
    sine_all = jnp.sin(angles)
    slab = 0
    field_f32 = (
        local_block[slab].reshape(eig_count, 2, 3, depth_planes, LXY, LXY).astype(jnp.float32)
    )
    widened_f32 = (
        extended[slab].reshape(eig_count, 2, 3, depth_planes + 2, LXY, LXY).astype(jnp.float32)
    )
    slab_links = gauge_links[slab].reshape(3, 2, 3, 3, depth_planes, LXY, LXY).astype(jnp.float32)
    prev_links = links_below[slab].reshape(2, 3, 3, depth_planes, LXY, LXY).astype(jnp.float32)
    per_dir = []
    for dir_index, roll_axis in ((0, -1), (1, -2)):
        forward = apply_link(slab_links[dir_index], jnp.roll(field_f32, -1, axis=roll_axis))
        backward = jnp.roll(
            apply_link(adjoint(slab_links[dir_index]), field_f32), 1, axis=roll_axis
        )
        per_dir.append(pack_terms(0.5 * (forward - backward), eig_count))
    forward = apply_link(slab_links[2], widened_f32[:, :, :, 2:])
    backward = apply_link(adjoint(prev_links), widened_f32[:, :, :, :depth_planes])
    per_dir.append(pack_terms(0.5 * (forward - backward), eig_count))
    packed_dirs = [per_dir]
    slab = 0
    row_block = local_block[slab]
    row_block = row_block.reshape(eig_count, 2, 3, depth_planes, LXY, LXY).astype(jnp.float32)
    per_mom = []
    for mom_first in range(0, NMOM, 2):
        twisted = phase_twist(
            row_block, cosine_all[mom_first : mom_first + 2], sine_all[mom_first : mom_first + 2]
        )
        per_dir = []
        for dir_index in range(3):
            product = lax.dot_general(
                twisted,
                packed_dirs[slab][dir_index],
                (((1,), (1,)), ((), ())),
                preferred_element_type=jnp.float32,
            )
            per_dir.append(product.reshape(2, eig_count, 2 * eig_count))
        per_mom.append(jnp.stack(per_dir, axis=2))
    mom_block = jnp.concatenate(per_mom, axis=0)
    per_slab = [jnp.transpose(mom_block, (1, 0, 2, 3))]
    summed = lax.psum_scatter(jnp.stack(per_slab, axis=1), "space", scatter_dimension=0, tiled=True)
    dir_select = (directions[:, None] == jnp.arange(NDIR, dtype=jnp.int32)[None, :]).astype(
        jnp.float32
    )
    return jnp.einsum("dm,itpmq->itpdq", dir_select, summed, precision=lax.Precision.HIGHEST)


LANES = 128


def add_links(link, rows, field, sign):
    real, imag = [], []
    for a in range(3):
        re_sum = im_sum = None
        for b in range(3):
            row = rows + (3 * a + b if sign > 0 else 3 * b + a)
            link_re, link_im = link(row), link(row + 9)
            re_b, im_b = field[b], field[3 + b]
            if sign > 0:
                re_t = link_re * re_b - link_im * im_b
                im_t = link_re * im_b + link_im * re_b
            else:
                re_t = link_re * re_b + link_im * im_b
                im_t = link_re * im_b - link_im * re_b
            re_sum = re_t if re_sum is None else re_sum + re_t
            im_sum = im_t if im_sum is None else im_sum + im_t
        real.append(re_sum)
        imag.append(im_sum)
    return real + imag


def spread(tiles, lane_group, roll):
    first = []
    for a, b in ((0, 1), (2, 3)):
        even = lane_group % 2 == 0
        first.append(jnp.where(even, tiles[a], roll(tiles[b], LXY)))
        first.append(jnp.where(even, roll(tiles[a], -LXY), tiles[b]))
    low = lane_group < 2
    out = [None] * 4
    for bit in range(2):
        near, far = first[bit], first[2 + bit]
        out[bit] = jnp.where(low, near, roll(far, 2 * LXY))
        out[2 + bit] = jnp.where(low, roll(near, -2 * LXY), far)
    return out


def kernel(
    count, depth, groups, field_ref, links_ref, momenta_ref, directions_ref, out_ref,
    local, stage, held, halo, held_links, wide_links, tab_ref, twisted, packed, packed_y, acc, acc_y, sent, got, sums,
    pay_send, pay_recv, halo_send, halo_recv, pass_send, pass_recv, link_send, link_recv, own_sem, part_send, part_recv,
):
    me = lax.axis_index("space")
    peers = lambda step: lax.rem(me + step, count)
    rows_of = field_ref.shape[3]
    eigs = count * rows_of
    moms = momenta_ref.shape[1]
    per_row = LANES // LXY
    pieces = depth // per_row
    row_k = 6 * pieces * LANES
    tall = count // 2
    half = lax.rem(me, 2)
    high = me // 2
    place_of = lambda device: lax.rem(device, 2) * (count - 1 - 2 * (device // 2)) + device // 2
    block = place_of(me)
    crossings = (tall // 2 - 1, tall + tall // 2 - 1)
    device_at = lambda place: 2 * place if place < tall else 2 * (count - 1 - place) + 1
    remote = lambda **rest: pltpu.make_async_remote_copy(device_id_type=pl.DeviceIdType.MESH, **rest)

    own_field = pltpu.make_async_copy(field_ref, local, own_sem.at[0])
    own_field.start()
    barrier = pltpu.get_barrier_semaphore()
    for step in range(1, count):
        pl.semaphore_signal(barrier, inc=1, device_id={"space": peers(step)}, device_id_type=pl.DeviceIdType.MESH)
    own_links = pltpu.make_async_copy(
        links_ref.at[:, :, pl.ds(pl.multiple_of(block * LANES, LANES), LANES)], held_links.at[me], own_sem.at[1]
    )
    own_links.start()

    def link_copy(target, source):
        return remote(
            src_ref=links_ref.at[:, :, pl.ds(pl.multiple_of(place_of(target) * LANES, LANES), LANES)],
            dst_ref=held_links.at[source],
            send_sem=link_send.at[target], recv_sem=link_recv.at[source], device_id={"space": target},
        )

    def pay_copy(row, target, source):
        return remote(
            src_ref=stage.at[place_of(target), row], dst_ref=held.at[row, source],
            send_sem=pay_send.at[row, target], recv_sem=pay_recv.at[row, source], device_id={"space": target},
        )

    def halo_copy(cross, source):
        place = crossings[cross]
        return remote(
            src_ref=stage.at[(place + 1) % count, 0], dst_ref=halo.at[source],
            send_sem=halo_send.at[cross], recv_sem=halo_recv.at[source], device_id={"space": device_at(place)},
        )

    def pass_copy():
        behind = lax.rem(block + count - 1, count)
        back = jnp.where(behind < tall, 2 * behind, 2 * (count - 1 - behind) + 1)
        return remote(
            src_ref=held.at[0], dst_ref=halo, send_sem=pass_send.at[0], recv_sem=pass_recv.at[0],
            device_id={"space": back},
        )

    def part_copy(group, target, source):
        span = pl.ds(group * (moms // groups), moms // groups)
        return remote(
            src_ref=sent.at[target, span], dst_ref=got.at[source, span],
            send_sem=part_send.at[group, target], recv_sem=part_recv.at[group, source], device_id={"space": target},
        )

    at_crossing = (block == crossings[0]) | (block == crossings[1])
    after_crossing = (block == crossings[0] + 1) | (block == (crossings[1] + 1) % count)
    roll = lambda value, shift: pltpu.roll(value, shift % LANES, 1)
    group_of = lambda rows: lax.broadcasted_iota(jnp.int32, (rows, LANES), 1) // LXY
    own_field.wait()

    def arrange(target, carry):
        lanes = group_of(rows_of)
        for c in range(6):
            for m in range(pieces):
                tiles = [local[c, m * per_row + q, target].astype(jnp.float32) for q in range(per_row)]
                for r, tile in enumerate(spread(tiles, lanes, roll)):
                    stage[target, r, c, m] = tile.astype(jnp.bfloat16)
        return carry

    lax.fori_loop(0, count, arrange, 0)
    pl.semaphore_wait(barrier, count - 1)

    for step in range(1, count):
        link_copy(peers(step), me).start()
    order = [0] + [d if s == 0 else tall - d for d in range(1, (tall + 1) // 2) for s in (0, 1)]
    if tall % 2 == 0:
        order.append(tall // 2)
    column = lambda hop: lax.rem(high + hop, tall)
    beside = [(hop, side) for hop in order for side in (1, 0)][:]
    beside.remove((0, 0))
    for row in range(per_row):
        for hop, side in beside:
            pay_copy(row, 2 * column(hop) + lax.rem(half + side, 2), me).start()
        if row == 1:
            for cross, place in enumerate(crossings):
                @pl.when(me != device_at(place))
                def _():
                    halo_copy(cross, me).start()
    for row in range(per_row):
        held[row, me] = stage[block, row]

    @pl.when(at_crossing)
    def _():
        halo[me] = stage[lax.rem(block + 1, count), 0]

    mom_row = lax.broadcasted_iota(jnp.int32, (moms, LANES), 0)
    mom_lane = lax.broadcasted_iota(jnp.int32, (moms, LANES), 1)
    moved = []
    for axis in range(3):
        values = jnp.zeros((moms, LANES), jnp.int32)
        for p in range(moms):
            values = jnp.where(mom_row == p, momenta_ref[axis, p], values)
        moved.append(values)
    part_x = ((moved[0] * (mom_lane % LXY)) & (LXY - 1)).astype(jnp.float32) / LXY
    for row in range(per_row + 1):
        for m in range(pieces):
            y_at = block * per_row + row
            z_at = m * per_row + mom_lane // LXY
            fraction = part_x + ((moved[1] * y_at) & (LXY - 1)).astype(jnp.float32) / LXY
            fraction = fraction + ((moved[2] * z_at) & (depth - 1)).astype(jnp.float32) / depth
            tab_ref[row * pieces + m, 0:moms] = jnp.cos(TWO_PI * fraction)
            tab_ref[row * pieces + m, moms:] = jnp.sin(TWO_PI * fraction)

    own_links.wait()
    for step in range(1, count):
        link_copy(peers(step), peers(step)).wait_recv()
    for m in range(pieces):
        for mu in range(NDIR):
            tiles = [held_links[m * per_row + q, mu].astype(jnp.float32) for q in range(per_row)]
            for r, tile in enumerate(spread(tiles, group_of(tiles[0].shape[0]), roll)):
                wide_links[r, m, mu] = 0.5 * tile

    wide = 2 * rows_of
    x_of = lax.rem(lax.broadcasted_iota(jnp.int32, (wide, LANES), 1), LXY)
    quarter = group_of(wide)

    def next_x(value):
        return jnp.where(x_of == LXY - 1, roll(value, LXY - 1), roll(value, -1))

    def last_x(value):
        return jnp.where(x_of == 0, roll(value, 1 - LXY), roll(value, 1))

    def links_at(row, m):
        return lambda entry: wide_links[row, m, entry // 18, entry % 18][None]

    def load_from(ref, pair, row, m):
        if row is None:
            return [ref[pl.ds(2 * pair, 2), c, m].astype(jnp.float32).reshape(wide, LANES) for c in range(6)]
        return [ref[row, pl.ds(2 * pair, 2), c, m].astype(jnp.float32).reshape(wide, LANES) for c in range(6)]

    def store_packed(ref, base, first, values, row, m):
        vals = [value.astype(jnp.bfloat16) for value in values]
        for c in range(6):
            span = pl.ds(row * row_k + (c * pieces + m) * LANES, LANES)
            ref[pl.ds(base + first, wide), span] = vals[c]
            ref[pl.ds(base + eigs + first, wide), span] = vals[c + 3] if c < 3 else -vals[c - 3]

    def twist(field, first, row, m):
        for p in range(moms):
            cosine = tab_ref[row * pieces + m, p][None]
            sine = tab_ref[row * pieces + m, moms + p][None]
            for c in range(3):
                real = field[c] * cosine - field[c + 3] * sine
                imag = field[c] * sine + field[c + 3] * cosine
                for part, value in ((c, real), (c + 3, imag)):
                    span = pl.ds(row * row_k + (part * pieces + m) * LANES, LANES)
                    twisted[pl.ds(p * eigs + first, wide), span] = value.astype(jnp.bfloat16)

    def along_y(pair, first, row, m):
        ahead = load_from(held, pair, row + 1, m) if row + 1 < per_row else load_from(halo, pair, None, m)
        values = add_links(links_at(row, m), 18, ahead, 1)
        if row:
            behind = add_links(links_at(row - 1, m), 18, load_from(held, pair, row - 1, m), -1)
            values = [f - b for f, b in zip(values, behind)]
        store_packed(packed_y, 0, first, values, row, m)

    def do_row(row, pair):
        first = pl.multiple_of(pair * wide, wide)
        behind = []
        for m in range(pieces):
            field = load_from(held, pair, row, m)
            twist(field, first, row, m)
            forward = add_links(links_at(row, m), 0, [next_x(v) for v in field], 1)
            backward = [last_x(v) for v in add_links(links_at(row, m), 0, field, -1)]
            store_packed(packed, 0, first, [f - b for f, b in zip(forward, backward)], row, m)
        for m in range(pieces):
            behind.append([roll(v, LXY) for v in add_links(links_at(row, m), 36, load_from(held, pair, row, m), -1)])
        for m in range(pieces):
            field, after = load_from(held, pair, row, m), load_from(held, pair, row, (m + 1) % pieces)
            shifted = [
                jnp.where(quarter == per_row - 1, roll(a, -LXY), roll(v, -LXY)) for v, a in zip(field, after)
            ]
            forward = add_links(links_at(row, m), 36, shifted, 1)
            backward = [
                jnp.where(quarter == 0, a, b) for a, b in zip(behind[(m - 1) % pieces], behind[m])
            ]
            store_packed(packed, 2 * eigs, first, [f - b for f, b in zip(forward, backward)], row, m)
        if row:
            for m in range(pieces):
                along_y(pair, first, row - 1, m)
        if row == per_row - 1:
            for m in range(pieces):
                along_y(pair, first, row, m)
                tails = add_links(links_at(row, m), 18, load_from(held, pair, row, m), -1)
                store_packed(packed_y, 0, first, [-v for v in tails], row + 1, m)

    contract = (((1,), (1,)), ((), ()))

    def dot_of(rows, ref, first_row, last_row):
        span = slice(first_row * row_k, last_row * row_k)
        return lax.dot_general(twisted[rows, span], ref[:, span], contract, preferred_element_type=jnp.float32)

    every = slice(0, moms * eigs)
    for row in range(per_row):
        def one(i, carry):
            pair = column(jnp.where(i < 2, i, tall + 1 - i))
            for side in range(2):
                source = 2 * pair + side

                @pl.when(source != me)
                def _():
                    pay_copy(row, source, source).wait_recv()
            do_row(row, pair)
            return carry

        if row == per_row - 1:
            @pl.when(at_crossing)
            def _():
                for step in range(1, count):
                    halo_copy(0, peers(step)).wait_recv()

            @pl.when(jnp.logical_not(at_crossing))
            def _():
                pass_copy().wait_recv()

            def last(pair, carry):
                for m in range(pieces):
                    twist(load_from(halo, pair, None, m), pl.multiple_of(pair * wide, wide), per_row, m)
                return carry

            lax.fori_loop(0, tall, last, 0)
        lax.fori_loop(0, tall, one, 0)
        if row == 0:
            @pl.when(jnp.logical_not(after_crossing))
            def _():
                pass_copy().start()
        if row == 1:
            acc[...] = dot_of(every, packed, 0, 2)
        if row == 2:
            acc[...] += dot_of(every, packed, 2, 3)
            acc_y[...] = dot_of(every, packed_y, 0, 2)

    each = moms // groups
    width = 2 * eigs
    for group in range(groups):
        rows = slice(group * each * eigs, (group + 1) * each * eigs)
        along = acc[rows] + dot_of(rows, packed, per_row - 1, per_row)
        across = acc_y[rows] + dot_of(rows, packed_y, 2, per_row + 1)
        for d, result in enumerate((along[:, :width], across, along[:, width:])):
            result = result.reshape(each, count, rows_of, width)
            for p in range(each):
                for target in range(count):
                    sent[target, group * each + p, d] = result[p, target].astype(jnp.bfloat16)
        for step in range(1, count):
            part_copy(group, peers(step), me).start()

    got[me] = sent[me]
    for group in range(groups):
        for step in range(1, count):
            part_copy(group, peers(step), peers(step)).wait_recv()
        for p in range(group * each, (group + 1) * each):
            for d in range(NDIR):
                total = got[0, p, d].astype(jnp.float32)
                for source in range(1, count):
                    total = total + got[source, p, d].astype(jnp.float32)
                sums[d, p] = total
    for d in range(NDIR):
        for p in range(moms):
            out_ref[:, d, p] = sums[directions_ref[d], p]

    for step in range(1, count):
        target = peers(step)
        link_copy(target, me).wait_send()
        for row in range(per_row):
            pay_copy(row, target, me).wait_send()
        for group in range(groups):
            part_copy(group, target, me).wait_send()
    for cross, place in enumerate(crossings):
        @pl.when(me != device_at(place))
        def _():
            halo_copy(cross, me).wait_send()

    @pl.when(jnp.logical_not(after_crossing))
    def _():
        pass_copy().wait_send()


def shards_by_rows(vectors, gauge_links, momenta, directions):
    count = lax.axis_size("space")
    eig_local = vectors.shape[1]
    eigs = eig_local * count
    moms = momenta.shape[0]
    depth = vectors.shape[3] // (LXY * LXY)
    per_row = LANES // LXY
    pieces = depth // per_row
    field = jnp.transpose(vectors[0].reshape(eig_local, 6, depth, count, LANES), (1, 2, 3, 0, 4))

    groups = 2
    row_k = 6 * pieces * LANES
    vmem = pl.BlockSpec(memory_space=pltpu.VMEM)
    part = (count, moms, NDIR, eig_local, 2 * eigs)
    lump = (6, pieces, eig_local, LANES)
    summed = pl.pallas_call(
        lambda *refs: kernel(count, depth, groups, *refs),
        out_shape=jax.ShapeDtypeStruct((eig_local, NDIR, moms, 2 * eigs), jnp.float32),
        in_specs=[
            pl.BlockSpec(memory_space=pl.ANY),
            pl.BlockSpec(memory_space=pl.ANY),
            pl.BlockSpec(memory_space=pltpu.SMEM),
            pl.BlockSpec(memory_space=pltpu.SMEM),
        ],
        out_specs=vmem,
        scratch_shapes=[
            pltpu.VMEM(field.shape, jnp.bfloat16),
            pltpu.VMEM((count, per_row) + lump, jnp.bfloat16),
            pltpu.VMEM((per_row, count) + lump, jnp.bfloat16),
            pltpu.VMEM((count,) + lump, jnp.bfloat16),
            pltpu.VMEM((count, NDIR, 18, LANES), jnp.bfloat16),
            pltpu.VMEM((per_row, pieces, NDIR, 18, LANES), jnp.float32),
            pltpu.VMEM(((per_row + 1) * pieces, 2 * moms, LANES), jnp.float32),
            pltpu.VMEM((moms * eigs, (per_row + 1) * row_k), jnp.bfloat16),
            pltpu.VMEM((4 * eigs, per_row * row_k), jnp.bfloat16),
            pltpu.VMEM((2 * eigs, (per_row + 1) * row_k), jnp.bfloat16),
            pltpu.VMEM((moms * eigs, 4 * eigs), jnp.float32),
            pltpu.VMEM((moms * eigs, 2 * eigs), jnp.float32),
            pltpu.VMEM(part, jnp.bfloat16),
            pltpu.VMEM(part, jnp.bfloat16),
            pltpu.VMEM((NDIR, moms, eig_local, 2 * eigs), jnp.float32),
            pltpu.SemaphoreType.DMA((per_row, count)),
            pltpu.SemaphoreType.DMA((per_row, count)),
            pltpu.SemaphoreType.DMA((2,)),
            pltpu.SemaphoreType.DMA((count,)),
            pltpu.SemaphoreType.DMA((1,)),
            pltpu.SemaphoreType.DMA((1,)),
            pltpu.SemaphoreType.DMA((count,)),
            pltpu.SemaphoreType.DMA((count,)),
            pltpu.SemaphoreType.DMA((2,)),
            pltpu.SemaphoreType.DMA((groups, count)),
            pltpu.SemaphoreType.DMA((groups, count)),
        ],
        compiler_params=pltpu.CompilerParams(collective_id=0, has_side_effects=True),
        name="elementals",
    )(field, gauge_links[0], momenta.T, directions)
    return jnp.transpose(summed, (0, 2, 1, 3))[:, None]


def shards(vectors, gauge_links, momenta, directions):
    count = lax.axis_size("space")
    depth = vectors.shape[3] // (LXY * LXY)
    by_rows = (
        vectors.shape[0] == 1
        and count * LANES == LXY * LXY
        and depth == count
        and depth & (depth - 1) == 0
        and depth == 2 * (LANES // LXY)
        and vectors.shape[1] % 8 == 0
    )
    body = shards_by_rows if by_rows else shards_by_plane
    return body(vectors, gauge_links, momenta, directions)


def solution(mesh):
    return jax.shard_map(
        shards,
        mesh=mesh,
        in_specs=(
            P(("cfg", "tm"), "space", None, None),
            P(("cfg", "tm"), None, None, "space"),
            P(),
            P(),
        ),
        out_specs=P("space", ("cfg", "tm"), None, None, None),
        check_vma=False,
    )
```

```python
import math

import jax
import jax.numpy as jnp
from jax import lax
from jax.experimental import pallas as pl
from jax.experimental.pallas import tpu as pltpu
from jax.sharding import PartitionSpec as P

LXY = 32
NMOM = 8
NDIR = 3


TWO_PI = 2.0 * math.pi


def with_halo(cells, sides, width):
    for axis, dim in sides:
        count = lax.axis_size(axis)
        head = lax.slice_in_dim(cells, 0, width, axis=dim)
        tail = lax.slice_in_dim(cells, cells.shape[dim] - width, cells.shape[dim], axis=dim)
        cells = jnp.concatenate(
            [
                lax.ppermute(tail, axis, [(i, (i + 1) % count) for i in range(count)]),
                cells,
                lax.ppermute(head, axis, [((i + 1) % count, i) for i in range(count)]),
            ],
            axis=dim,
        )
    return cells


def from_behind(block, axis, distance):
    devices = range(lax.axis_size(axis))
    route = [((i - distance) % len(devices), i) for i in devices]
    return lax.ppermute(block, axis, route)


def apply_link(link, field_f32):
    real_rows = []
    imag_rows = []
    for row_a in range(3):
        link_re = link[0, row_a, 0][None]
        link_im = link[1, row_a, 0][None]
        real_acc = link_re * field_f32[:, 0, 0] - link_im * field_f32[:, 1, 0]
        imag_acc = link_re * field_f32[:, 1, 0] + link_im * field_f32[:, 0, 0]
        for col_b in range(1, 3):
            link_re = link[0, row_a, col_b][None]
            link_im = link[1, row_a, col_b][None]
            real_acc = (
                real_acc + link_re * field_f32[:, 0, col_b] - link_im * field_f32[:, 1, col_b]
            )
            imag_acc = (
                imag_acc + link_re * field_f32[:, 1, col_b] + link_im * field_f32[:, 0, col_b]
            )
        real_rows.append(real_acc)
        imag_rows.append(imag_acc)
    return jnp.stack([jnp.stack(real_rows, axis=1), jnp.stack(imag_rows, axis=1)], axis=1)


def adjoint(link):
    return jnp.stack([jnp.swapaxes(link[0], 0, 1), -jnp.swapaxes(link[1], 0, 1)])


def pack_terms(derivative, eig_count):
    rounded = derivative.astype(jnp.bfloat16)
    rounded_re = rounded[:, 0]
    rounded_im = rounded[:, 1]
    swapped = jnp.stack([rounded_im, -rounded_re], axis=1)
    return jnp.concatenate([rounded, swapped], axis=0).reshape(2 * eig_count, -1)


def phase_angles(momenta, z_offset, depth_planes, z_length):
    z_coord = z_offset + jnp.arange(depth_planes, dtype=jnp.int32)
    y_coord = jnp.arange(LXY, dtype=jnp.int32)
    x_coord = jnp.arange(LXY, dtype=jnp.int32)
    mom_x = momenta[:, 0][:, None, None, None]
    mom_y = momenta[:, 1][:, None, None, None]
    mom_z = momenta[:, 2][:, None, None, None]
    fraction = (mom_x * x_coord[None, None, None, :] % LXY).astype(jnp.float32) / LXY
    fraction = fraction + (mom_y * y_coord[None, None, :, None] % LXY).astype(jnp.float32) / LXY
    fraction = (
        fraction + (mom_z * z_coord[None, :, None, None] % z_length).astype(jnp.float32) / z_length
    )
    return TWO_PI * fraction


def phase_twist(row_block, cosine_table, sine_table):
    vec_re = row_block[:, 0][None]
    vec_im = row_block[:, 1][None]
    cos_b = cosine_table[:, None, None]
    sin_b = sine_table[:, None, None]
    real_part = vec_re * cos_b - vec_im * sin_b
    imag_part = vec_re * sin_b + vec_im * cos_b
    twisted = jnp.stack([real_part, imag_part], axis=2).astype(jnp.bfloat16)
    return twisted.reshape(cosine_table.shape[0] * row_block.shape[0], -1)


def shards_by_plane(vectors, gauge_links, momenta, directions):
    space_count = lax.axis_size("space")
    slab_count = vectors.shape[0]
    eig_local = vectors.shape[1]
    eig_count = eig_local * space_count
    plane_size = LXY * LXY
    depth_planes = gauge_links.shape[3] // plane_size
    blocks = vectors.reshape(slab_count, eig_local, 6, space_count, depth_planes, plane_size)
    regrouped = lax.all_to_all(blocks, "space", split_axis=3, concat_axis=1, tiled=True)
    local_block = regrouped.reshape(slab_count, eig_count, 6, depth_planes, plane_size)
    extended = with_halo(local_block, (("space", 3),), 1)
    z_links = gauge_links[:, 2].reshape(slab_count, 18, depth_planes, plane_size)
    link_below = from_behind(z_links[:, :, depth_planes - 1, :], "space", 1)
    links_below = jnp.concatenate(
        [link_below[:, :, None, :], z_links[:, :, : depth_planes - 1, :]], axis=2
    )
    z_offset = lax.axis_index("space") * depth_planes
    angles = phase_angles(momenta, z_offset, depth_planes, depth_planes * space_count)
    cosine_all = jnp.cos(angles)
    sine_all = jnp.sin(angles)
    slab = 0
    field_f32 = (
        local_block[slab].reshape(eig_count, 2, 3, depth_planes, LXY, LXY).astype(jnp.float32)
    )
    widened_f32 = (
        extended[slab].reshape(eig_count, 2, 3, depth_planes + 2, LXY, LXY).astype(jnp.float32)
    )
    slab_links = gauge_links[slab].reshape(3, 2, 3, 3, depth_planes, LXY, LXY).astype(jnp.float32)
    prev_links = links_below[slab].reshape(2, 3, 3, depth_planes, LXY, LXY).astype(jnp.float32)
    per_dir = []
    for dir_index, roll_axis in ((0, -1), (1, -2)):
        forward = apply_link(slab_links[dir_index], jnp.roll(field_f32, -1, axis=roll_axis))
        backward = jnp.roll(
            apply_link(adjoint(slab_links[dir_index]), field_f32), 1, axis=roll_axis
        )
        per_dir.append(pack_terms(0.5 * (forward - backward), eig_count))
    forward = apply_link(slab_links[2], widened_f32[:, :, :, 2:])
    backward = apply_link(adjoint(prev_links), widened_f32[:, :, :, :depth_planes])
    per_dir.append(pack_terms(0.5 * (forward - backward), eig_count))
    packed_dirs = [per_dir]
    slab = 0
    row_block = local_block[slab]
    row_block = row_block.reshape(eig_count, 2, 3, depth_planes, LXY, LXY).astype(jnp.float32)
    per_mom = []
    for mom_first in range(0, NMOM, 2):
        twisted = phase_twist(
            row_block, cosine_all[mom_first : mom_first + 2], sine_all[mom_first : mom_first + 2]
        )
        per_dir = []
        for dir_index in range(3):
            product = lax.dot_general(
                twisted,
                packed_dirs[slab][dir_index],
                (((1,), (1,)), ((), ())),
                preferred_element_type=jnp.float32,
            )
            per_dir.append(product.reshape(2, eig_count, 2 * eig_count))
        per_mom.append(jnp.stack(per_dir, axis=2))
    mom_block = jnp.concatenate(per_mom, axis=0)
    per_slab = [jnp.transpose(mom_block, (1, 0, 2, 3))]
    summed = lax.psum_scatter(jnp.stack(per_slab, axis=1), "space", scatter_dimension=0, tiled=True)
    dir_select = (directions[:, None] == jnp.arange(NDIR, dtype=jnp.int32)[None, :]).astype(
        jnp.float32
    )
    return jnp.einsum("dm,itpmq->itpdq", dir_select, summed, precision=lax.Precision.HIGHEST)


LANES = 128


def add_links(link, rows, field, sign):
    real, imag = [], []
    for a in range(3):
        re_sum = im_sum = None
        for b in range(3):
            row = rows + (3 * a + b if sign > 0 else 3 * b + a)
            link_re, link_im = link(row), link(row + 9)
            re_b, im_b = field[b], field[3 + b]
            if sign > 0:
                re_t = link_re * re_b - link_im * im_b
                im_t = link_re * im_b + link_im * re_b
            else:
                re_t = link_re * re_b + link_im * im_b
                im_t = link_re * im_b - link_im * re_b
            re_sum = re_t if re_sum is None else re_sum + re_t
            im_sum = im_t if im_sum is None else im_sum + im_t
        real.append(re_sum)
        imag.append(im_sum)
    return real + imag


def spread(tiles, lane_group, roll):
    first = []
    for a, b in ((0, 1), (2, 3)):
        even = lane_group % 2 == 0
        first.append(jnp.where(even, tiles[a], roll(tiles[b], LXY)))
        first.append(jnp.where(even, roll(tiles[a], -LXY), tiles[b]))
    low = lane_group < 2
    out = [None] * 4
    for bit in range(2):
        near, far = first[bit], first[2 + bit]
        out[bit] = jnp.where(low, near, roll(far, 2 * LXY))
        out[2 + bit] = jnp.where(low, roll(near, -2 * LXY), far)
    return out


def kernel(
    count, depth, groups, field_ref, links_ref, momenta_ref, directions_ref, out_ref,
    local, stage, held, halo, held_links, wide_links, tab_ref, twisted, packed, packed_y, acc, acc_y, sent, got, sent_y, got_y, sums,
    pay_send, pay_recv, halo_send, halo_recv, pass_send, pass_recv, link_send, link_recv, own_sem, part_send, part_recv,
):
    me = lax.axis_index("space")
    peers = lambda step: lax.rem(me + step, count)
    rows_of = field_ref.shape[3]
    eigs = count * rows_of
    moms = momenta_ref.shape[1]
    per_row = LANES // LXY
    pieces = depth // per_row
    row_k = 6 * pieces * LANES
    tall = count // 2
    half = lax.rem(me, 2)
    high = me // 2
    place_of = lambda device: lax.rem(device, 2) * (count - 1 - 2 * (device // 2)) + device // 2
    block = place_of(me)
    crossings = (tall // 2 - 1, tall + tall // 2 - 1)
    device_at = lambda place: 2 * place if place < tall else 2 * (count - 1 - place) + 1
    remote = lambda **rest: pltpu.make_async_remote_copy(device_id_type=pl.DeviceIdType.MESH, **rest)

    own_field = pltpu.make_async_copy(field_ref, local, own_sem.at[0])
    own_field.start()
    barrier = pltpu.get_barrier_semaphore()
    for step in range(1, count):
        pl.semaphore_signal(barrier, inc=1, device_id={"space": peers(step)}, device_id_type=pl.DeviceIdType.MESH)
    own_links = pltpu.make_async_copy(
        links_ref.at[:, :, pl.ds(pl.multiple_of(block * LANES, LANES), LANES)], held_links.at[me], own_sem.at[1]
    )
    own_links.start()

    def link_copy(target, source):
        return remote(
            src_ref=links_ref.at[:, :, pl.ds(pl.multiple_of(place_of(target) * LANES, LANES), LANES)],
            dst_ref=held_links.at[source],
            send_sem=link_send.at[target], recv_sem=link_recv.at[source], device_id={"space": target},
        )

    def pay_copy(row, target, source):
        return remote(
            src_ref=stage.at[place_of(target), row], dst_ref=held.at[row, source],
            send_sem=pay_send.at[row, target], recv_sem=pay_recv.at[row, source], device_id={"space": target},
        )

    def halo_copy(cross, source):
        place = crossings[cross]
        return remote(
            src_ref=stage.at[(place + 1) % count, 0], dst_ref=halo.at[source],
            send_sem=halo_send.at[cross], recv_sem=halo_recv.at[source], device_id={"space": device_at(place)},
        )

    def pass_copy():
        behind = lax.rem(block + count - 1, count)
        back = jnp.where(behind < tall, 2 * behind, 2 * (count - 1 - behind) + 1)
        return remote(
            src_ref=held.at[0], dst_ref=halo, send_sem=pass_send.at[0], recv_sem=pass_recv.at[0],
            device_id={"space": back},
        )

    def part_copy(group, target, source):
        return remote(
            src_ref=(sent, sent_y)[group].at[target], dst_ref=(got, got_y)[group].at[source],
            send_sem=part_send.at[group, target], recv_sem=part_recv.at[group, source], device_id={"space": target},
        )

    at_crossing = (block == crossings[0]) | (block == crossings[1])
    after_crossing = (block == crossings[0] + 1) | (block == (crossings[1] + 1) % count)
    roll = lambda value, shift: pltpu.roll(value, shift % LANES, 1)
    group_of = lambda rows: lax.broadcasted_iota(jnp.int32, (rows, LANES), 1) // LXY
    own_field.wait()

    def arrange(target, carry):
        lanes = group_of(rows_of)
        for c in range(6):
            for m in range(pieces):
                tiles = [local[c, m * per_row + q, target].astype(jnp.float32) for q in range(per_row)]
                for r, tile in enumerate(spread(tiles, lanes, roll)):
                    stage[target, r, c, m] = tile.astype(jnp.bfloat16)
        return carry

    lax.fori_loop(0, count, arrange, 0)
    pl.semaphore_wait(barrier, count - 1)

    for step in range(1, count):
        link_copy(peers(step), me).start()
    order = [0] + [d if s == 0 else tall - d for d in range(1, (tall + 1) // 2) for s in (0, 1)]
    if tall % 2 == 0:
        order.append(tall // 2)
    column = lambda hop: lax.rem(high + hop, tall)
    beside = [(hop, side) for hop in order for side in (1, 0)][:]
    beside.remove((0, 0))
    far = sorted(beside, key=lambda hop: -min(hop[0], tall - hop[0]))
    outer = (high == 0) | (high == tall - 1)

    def send_row(row):
        for hop, side in far:
            pay_copy(row, 2 * column(hop) + lax.rem(half + side, 2), me).start()

    send_row(0)
    send_row(1)
    for cross, place in enumerate(crossings):
        @pl.when(me != device_at(place))
        def _():
            halo_copy(cross, me).start()

    @pl.when(jnp.logical_not(outer))
    def _():
        for row in range(2, per_row):
            send_row(row)

    for row in range(per_row):
        held[row, me] = stage[block, row]

    @pl.when(at_crossing)
    def _():
        halo[me] = stage[lax.rem(block + 1, count), 0]

    mom_row = lax.broadcasted_iota(jnp.int32, (moms, LANES), 0)
    mom_lane = lax.broadcasted_iota(jnp.int32, (moms, LANES), 1)
    moved = []
    for axis in range(3):
        values = jnp.zeros((moms, LANES), jnp.int32)
        for p in range(moms):
            values = jnp.where(mom_row == p, momenta_ref[axis, p], values)
        moved.append(values)
    part_x = ((moved[0] * (mom_lane % LXY)) & (LXY - 1)).astype(jnp.float32) / LXY
    for row in range(per_row + 1):
        for m in range(pieces):
            y_at = block * per_row + row
            z_at = m * per_row + mom_lane // LXY
            fraction = part_x + ((moved[1] * y_at) & (LXY - 1)).astype(jnp.float32) / LXY
            fraction = fraction + ((moved[2] * z_at) & (depth - 1)).astype(jnp.float32) / depth
            tab_ref[row * pieces + m, 0:moms] = jnp.cos(TWO_PI * fraction)
            tab_ref[row * pieces + m, moms:] = jnp.sin(TWO_PI * fraction)

    own_links.wait()
    for step in range(1, count):
        link_copy(peers(step), peers(step)).wait_recv()
    for m in range(pieces):
        for mu in range(NDIR):
            tiles = [held_links[m * per_row + q, mu].astype(jnp.float32) for q in range(per_row)]
            for r, tile in enumerate(spread(tiles, group_of(tiles[0].shape[0]), roll)):
                wide_links[r, m, mu] = 0.5 * tile

    wide = 2 * rows_of
    x_of = lax.rem(lax.broadcasted_iota(jnp.int32, (wide, LANES), 1), LXY)
    quarter = group_of(wide)

    def next_x(value):
        return jnp.where(x_of == LXY - 1, roll(value, LXY - 1), roll(value, -1))

    def last_x(value):
        return jnp.where(x_of == 0, roll(value, 1 - LXY), roll(value, 1))

    def links_at(row, m):
        return lambda entry: wide_links[row, m, entry // 18, entry % 18][None]

    def load_from(ref, pair, row, m):
        if row is None:
            return [ref[pl.ds(2 * pair, 2), c, m].astype(jnp.float32).reshape(wide, LANES) for c in range(6)]
        return [ref[row, pl.ds(2 * pair, 2), c, m].astype(jnp.float32).reshape(wide, LANES) for c in range(6)]

    def store_packed(ref, base, first, values, row, m):
        vals = [value.astype(jnp.bfloat16) for value in values]
        for c in range(6):
            span = pl.ds(row * row_k + (c * pieces + m) * LANES, LANES)
            ref[pl.ds(base + first, wide), span] = vals[c]
            ref[pl.ds(base + eigs + first, wide), span] = vals[c + 3] if c < 3 else -vals[c - 3]

    def twist(field, first, row, m):
        for p in range(moms):
            cosine = tab_ref[row * pieces + m, p][None]
            sine = tab_ref[row * pieces + m, moms + p][None]
            for c in range(3):
                real = field[c] * cosine - field[c + 3] * sine
                imag = field[c] * sine + field[c + 3] * cosine
                for part, value in ((c, real), (c + 3, imag)):
                    span = pl.ds(row * row_k + (part * pieces + m) * LANES, LANES)
                    twisted[pl.ds(p * eigs + first, wide), span] = value.astype(jnp.bfloat16)

    def along_y(pair, first, row, m):
        ahead = load_from(held, pair, row + 1, m) if row + 1 < per_row else load_from(halo, pair, None, m)
        values = add_links(links_at(row, m), 18, ahead, 1)
        if row:
            behind = add_links(links_at(row - 1, m), 18, load_from(held, pair, row - 1, m), -1)
            values = [f - b for f, b in zip(values, behind)]
        store_packed(packed_y, 0, first, values, row, m)

    def do_row(row, pair):
        first = pl.multiple_of(pair * wide, wide)
        behind = []
        for m in range(pieces):
            field = load_from(held, pair, row, m)
            twist(field, first, row, m)
            forward = add_links(links_at(row, m), 0, [next_x(v) for v in field], 1)
            backward = [last_x(v) for v in add_links(links_at(row, m), 0, field, -1)]
            store_packed(packed, 0, first, [f - b for f, b in zip(forward, backward)], row, m)
        for m in range(pieces):
            behind.append([roll(v, LXY) for v in add_links(links_at(row, m), 36, load_from(held, pair, row, m), -1)])
        for m in range(pieces):
            field, after = load_from(held, pair, row, m), load_from(held, pair, row, (m + 1) % pieces)
            shifted = [
                jnp.where(quarter == per_row - 1, roll(a, -LXY), roll(v, -LXY)) for v, a in zip(field, after)
            ]
            forward = add_links(links_at(row, m), 36, shifted, 1)
            backward = [
                jnp.where(quarter == 0, a, b) for a, b in zip(behind[(m - 1) % pieces], behind[m])
            ]
            store_packed(packed, 2 * eigs, first, [f - b for f, b in zip(forward, backward)], row, m)
        if 0 < row < per_row - 1:
            for m in range(pieces):
                along_y(pair, first, row - 1, m)

    def finish_y(pair, carry):
        first = pl.multiple_of(pair * wide, wide)
        for m in range(pieces):
            along_y(pair, first, per_row - 2, m)
            along_y(pair, first, per_row - 1, m)
            tails = add_links(links_at(per_row - 1, m), 18, load_from(held, pair, per_row - 1, m), -1)
            store_packed(packed_y, 0, first, [-v for v in tails], per_row, m)
        return carry

    contract = (((1,), (1,)), ((), ()))

    def dot_of(rows, ref, first_row, last_row):
        span = slice(first_row * row_k, last_row * row_k)
        middle = (rows.start + rows.stop) // 2
        parts = [
            lax.dot_general(twisted[part, span], ref[:, span], contract, preferred_element_type=jnp.float32)
            for part in (slice(rows.start, middle), slice(middle, rows.stop))
        ]
        return jnp.concatenate(parts, axis=0)

    every = slice(0, moms * eigs)
    for row in range(per_row):
        def one(i, carry):
            pair = column(jnp.where(i < 2, i, tall + 1 - i))
            for side in range(2):
                source = 2 * pair + side

                @pl.when(source != me)
                def _():
                    pay_copy(row, source, source).wait_recv()
            do_row(row, pair)
            return carry

        lax.fori_loop(0, tall, one, 0)
        if row + 2 < per_row:
            @pl.when(outer)
            def _():
                send_row(row + 2)
        if row == 0:
            @pl.when(jnp.logical_not(after_crossing))
            def _():
                pass_copy().start()
            acc[...] = dot_of(every, packed, 0, 1)
        if row == 1:
            acc[...] += dot_of(every, packed, 1, 2)
            acc_y[...] = dot_of(every, packed_y, 0, 1)
        if row == 2:
            acc[...] += dot_of(every, packed, 2, 3)
        if row == 1:
            @pl.when(at_crossing)
            def _():
                for step in range(1, count):
                    halo_copy(0, peers(step)).wait_recv()

            @pl.when(jnp.logical_not(at_crossing))
            def _():
                pass_copy().wait_recv()

            def last(pair, carry):
                for m in range(pieces):
                    twist(load_from(halo, pair, None, m), pl.multiple_of(pair * wide, wide), per_row, m)
                return carry

            lax.fori_loop(0, tall, last, 0)

    width = 2 * eigs

    def scatter(group, result, index):
        result = result.reshape(moms, count, rows_of, width)
        for p in range(moms):
            for target in range(count):
                (sent, sent_y)[group][(target, p) + index] = result[p, target].astype(jnp.bfloat16)

    along = acc[...] + dot_of(every, packed, per_row - 1, per_row)
    for d in range(2):
        scatter(0, along[:, d * width : (d + 1) * width], (d,))
    reach = [2 * column(hop) + lax.rem(half + side, 2) for hop, side in far]
    for target in reach:
        part_copy(0, target, me).start()
    lax.fori_loop(0, tall, finish_y, 0)
    scatter(1, acc_y[...] + dot_of(every, packed_y, 1, per_row + 1), ())
    for target in reach:
        part_copy(1, target, me).start()

    got[me] = sent[me]
    got_y[me] = sent_y[me]
    for group in range(groups):
        for step in range(1, count):
            part_copy(group, peers(step), peers(step)).wait_recv()
        for p in range(moms):
            for d in range(2 - group):
                at = (p, d) if group == 0 else (p,)
                buffer = (got, got_y)[group]
                total = buffer[(0,) + at].astype(jnp.float32)
                for source in range(1, count):
                    total = total + buffer[(source,) + at].astype(jnp.float32)
                sums[2 * d if group == 0 else 1, p] = total
    for d in range(NDIR):
        for p in range(moms):
            out_ref[:, d, p] = sums[directions_ref[d], p]

    for step in range(1, count):
        target = peers(step)
        link_copy(target, me).wait_send()
        for row in range(per_row):
            pay_copy(row, target, me).wait_send()
        for group in range(groups):
            part_copy(group, target, me).wait_send()
    for cross, place in enumerate(crossings):
        @pl.when(me != device_at(place))
        def _():
            halo_copy(cross, me).wait_send()

    @pl.when(jnp.logical_not(after_crossing))
    def _():
        pass_copy().wait_send()


def shards_by_rows(vectors, gauge_links, momenta, directions):
    count = lax.axis_size("space")
    eig_local = vectors.shape[1]
    eigs = eig_local * count
    moms = momenta.shape[0]
    depth = vectors.shape[3] // (LXY * LXY)
    per_row = LANES // LXY
    pieces = depth // per_row
    field = jnp.transpose(vectors[0].reshape(eig_local, 6, depth, count, LANES), (1, 2, 3, 0, 4))

    groups = 2
    row_k = 6 * pieces * LANES
    vmem = pl.BlockSpec(memory_space=pltpu.VMEM)
    part = (count, moms, 2, eig_local, 2 * eigs)
    part_y = (count, moms, eig_local, 2 * eigs)
    lump = (6, pieces, eig_local, LANES)
    summed = pl.pallas_call(
        lambda *refs: kernel(count, depth, groups, *refs),
        out_shape=jax.ShapeDtypeStruct((eig_local, NDIR, moms, 2 * eigs), jnp.float32),
        in_specs=[
            pl.BlockSpec(memory_space=pl.ANY),
            pl.BlockSpec(memory_space=pl.ANY),
            pl.BlockSpec(memory_space=pltpu.SMEM),
            pl.BlockSpec(memory_space=pltpu.SMEM),
        ],
        out_specs=vmem,
        scratch_shapes=[
            pltpu.VMEM(field.shape, jnp.bfloat16),
            pltpu.VMEM((count, per_row) + lump, jnp.bfloat16),
            pltpu.VMEM((per_row, count) + lump, jnp.bfloat16),
            pltpu.VMEM((count,) + lump, jnp.bfloat16),
            pltpu.VMEM((count, NDIR, 18, LANES), jnp.bfloat16),
            pltpu.VMEM((per_row, pieces, NDIR, 18, LANES), jnp.float32),
            pltpu.VMEM(((per_row + 1) * pieces, 2 * moms, LANES), jnp.float32),
            pltpu.VMEM((moms * eigs, (per_row + 1) * row_k), jnp.bfloat16),
            pltpu.VMEM((4 * eigs, per_row * row_k), jnp.bfloat16),
            pltpu.VMEM((2 * eigs, (per_row + 1) * row_k), jnp.bfloat16),
            pltpu.VMEM((moms * eigs, 4 * eigs), jnp.float32),
            pltpu.VMEM((moms * eigs, 2 * eigs), jnp.float32),
            pltpu.VMEM(part, jnp.bfloat16),
            pltpu.VMEM(part, jnp.bfloat16),
            pltpu.VMEM(part_y, jnp.bfloat16),
            pltpu.VMEM(part_y, jnp.bfloat16),
            pltpu.VMEM((NDIR, moms, eig_local, 2 * eigs), jnp.float32),
            pltpu.SemaphoreType.DMA((per_row, count)),
            pltpu.SemaphoreType.DMA((per_row, count)),
            pltpu.SemaphoreType.DMA((2,)),
            pltpu.SemaphoreType.DMA((count,)),
            pltpu.SemaphoreType.DMA((1,)),
            pltpu.SemaphoreType.DMA((1,)),
            pltpu.SemaphoreType.DMA((count,)),
            pltpu.SemaphoreType.DMA((count,)),
            pltpu.SemaphoreType.DMA((2,)),
            pltpu.SemaphoreType.DMA((groups, count)),
            pltpu.SemaphoreType.DMA((groups, count)),
        ],
        compiler_params=pltpu.CompilerParams(collective_id=0, has_side_effects=True),
        name="elementals",
    )(field, gauge_links[0], momenta.T, directions)
    return jnp.transpose(summed, (0, 2, 1, 3))[:, None]


def shards(vectors, gauge_links, momenta, directions):
    count = lax.axis_size("space")
    depth = vectors.shape[3] // (LXY * LXY)
    by_rows = (
        vectors.shape[0] == 1
        and count * LANES == LXY * LXY
        and depth == count
        and depth & (depth - 1) == 0
        and depth == 2 * (LANES // LXY)
        and vectors.shape[1] % 8 == 0
    )
    body = shards_by_rows if by_rows else shards_by_plane
    return body(vectors, gauge_links, momenta, directions)


def solution(mesh):
    return jax.shard_map(
        shards,
        mesh=mesh,
        in_specs=(
            P(("cfg", "tm"), "space", None, None),
            P(("cfg", "tm"), None, None, "space"),
            P(),
            P(),
        ),
        out_specs=P("space", ("cfg", "tm"), None, None, None),
        check_vma=False,
    )
```

```python
import math

import jax
import jax.numpy as jnp
from jax import lax
from jax.experimental import pallas as pl
from jax.experimental.pallas import tpu as pltpu
from jax.sharding import PartitionSpec as P

LXY = 32
NMOM = 8
NDIR = 3


TWO_PI = 2.0 * math.pi


def with_halo(cells, sides, width):
    for axis, dim in sides:
        count = lax.axis_size(axis)
        head = lax.slice_in_dim(cells, 0, width, axis=dim)
        tail = lax.slice_in_dim(cells, cells.shape[dim] - width, cells.shape[dim], axis=dim)
        cells = jnp.concatenate(
            [
                lax.ppermute(tail, axis, [(i, (i + 1) % count) for i in range(count)]),
                cells,
                lax.ppermute(head, axis, [((i + 1) % count, i) for i in range(count)]),
            ],
            axis=dim,
        )
    return cells


def from_behind(block, axis, distance):
    devices = range(lax.axis_size(axis))
    route = [((i - distance) % len(devices), i) for i in devices]
    return lax.ppermute(block, axis, route)


def apply_link(link, field_f32):
    real_rows = []
    imag_rows = []
    for row_a in range(3):
        link_re = link[0, row_a, 0][None]
        link_im = link[1, row_a, 0][None]
        real_acc = link_re * field_f32[:, 0, 0] - link_im * field_f32[:, 1, 0]
        imag_acc = link_re * field_f32[:, 1, 0] + link_im * field_f32[:, 0, 0]
        for col_b in range(1, 3):
            link_re = link[0, row_a, col_b][None]
            link_im = link[1, row_a, col_b][None]
            real_acc = (
                real_acc + link_re * field_f32[:, 0, col_b] - link_im * field_f32[:, 1, col_b]
            )
            imag_acc = (
                imag_acc + link_re * field_f32[:, 1, col_b] + link_im * field_f32[:, 0, col_b]
            )
        real_rows.append(real_acc)
        imag_rows.append(imag_acc)
    return jnp.stack([jnp.stack(real_rows, axis=1), jnp.stack(imag_rows, axis=1)], axis=1)


def adjoint(link):
    return jnp.stack([jnp.swapaxes(link[0], 0, 1), -jnp.swapaxes(link[1], 0, 1)])


def pack_terms(derivative, eig_count):
    rounded = derivative.astype(jnp.bfloat16)
    rounded_re = rounded[:, 0]
    rounded_im = rounded[:, 1]
    swapped = jnp.stack([rounded_im, -rounded_re], axis=1)
    return jnp.concatenate([rounded, swapped], axis=0).reshape(2 * eig_count, -1)


def phase_angles(momenta, z_offset, depth_planes, z_length):
    z_coord = z_offset + jnp.arange(depth_planes, dtype=jnp.int32)
    y_coord = jnp.arange(LXY, dtype=jnp.int32)
    x_coord = jnp.arange(LXY, dtype=jnp.int32)
    mom_x = momenta[:, 0][:, None, None, None]
    mom_y = momenta[:, 1][:, None, None, None]
    mom_z = momenta[:, 2][:, None, None, None]
    fraction = (mom_x * x_coord[None, None, None, :] % LXY).astype(jnp.float32) / LXY
    fraction = fraction + (mom_y * y_coord[None, None, :, None] % LXY).astype(jnp.float32) / LXY
    fraction = (
        fraction + (mom_z * z_coord[None, :, None, None] % z_length).astype(jnp.float32) / z_length
    )
    return TWO_PI * fraction


def phase_twist(row_block, cosine_table, sine_table):
    vec_re = row_block[:, 0][None]
    vec_im = row_block[:, 1][None]
    cos_b = cosine_table[:, None, None]
    sin_b = sine_table[:, None, None]
    real_part = vec_re * cos_b - vec_im * sin_b
    imag_part = vec_re * sin_b + vec_im * cos_b
    twisted = jnp.stack([real_part, imag_part], axis=2).astype(jnp.bfloat16)
    return twisted.reshape(cosine_table.shape[0] * row_block.shape[0], -1)


def shards_by_plane(vectors, gauge_links, momenta, directions):
    space_count = lax.axis_size("space")
    slab_count = vectors.shape[0]
    eig_local = vectors.shape[1]
    eig_count = eig_local * space_count
    plane_size = LXY * LXY
    depth_planes = gauge_links.shape[3] // plane_size
    blocks = vectors.reshape(slab_count, eig_local, 6, space_count, depth_planes, plane_size)
    regrouped = lax.all_to_all(blocks, "space", split_axis=3, concat_axis=1, tiled=True)
    local_block = regrouped.reshape(slab_count, eig_count, 6, depth_planes, plane_size)
    extended = with_halo(local_block, (("space", 3),), 1)
    z_links = gauge_links[:, 2].reshape(slab_count, 18, depth_planes, plane_size)
    link_below = from_behind(z_links[:, :, depth_planes - 1, :], "space", 1)
    links_below = jnp.concatenate(
        [link_below[:, :, None, :], z_links[:, :, : depth_planes - 1, :]], axis=2
    )
    z_offset = lax.axis_index("space") * depth_planes
    angles = phase_angles(momenta, z_offset, depth_planes, depth_planes * space_count)
    cosine_all = jnp.cos(angles)
    sine_all = jnp.sin(angles)
    slab = 0
    field_f32 = (
        local_block[slab].reshape(eig_count, 2, 3, depth_planes, LXY, LXY).astype(jnp.float32)
    )
    widened_f32 = (
        extended[slab].reshape(eig_count, 2, 3, depth_planes + 2, LXY, LXY).astype(jnp.float32)
    )
    slab_links = gauge_links[slab].reshape(3, 2, 3, 3, depth_planes, LXY, LXY).astype(jnp.float32)
    prev_links = links_below[slab].reshape(2, 3, 3, depth_planes, LXY, LXY).astype(jnp.float32)
    per_dir = []
    for dir_index, roll_axis in ((0, -1), (1, -2)):
        forward = apply_link(slab_links[dir_index], jnp.roll(field_f32, -1, axis=roll_axis))
        backward = jnp.roll(
            apply_link(adjoint(slab_links[dir_index]), field_f32), 1, axis=roll_axis
        )
        per_dir.append(pack_terms(0.5 * (forward - backward), eig_count))
    forward = apply_link(slab_links[2], widened_f32[:, :, :, 2:])
    backward = apply_link(adjoint(prev_links), widened_f32[:, :, :, :depth_planes])
    per_dir.append(pack_terms(0.5 * (forward - backward), eig_count))
    packed_dirs = [per_dir]
    slab = 0
    row_block = local_block[slab]
    row_block = row_block.reshape(eig_count, 2, 3, depth_planes, LXY, LXY).astype(jnp.float32)
    per_mom = []
    for mom_first in range(0, NMOM, 2):
        twisted = phase_twist(
            row_block, cosine_all[mom_first : mom_first + 2], sine_all[mom_first : mom_first + 2]
        )
        per_dir = []
        for dir_index in range(3):
            product = lax.dot_general(
                twisted,
                packed_dirs[slab][dir_index],
                (((1,), (1,)), ((), ())),
                preferred_element_type=jnp.float32,
            )
            per_dir.append(product.reshape(2, eig_count, 2 * eig_count))
        per_mom.append(jnp.stack(per_dir, axis=2))
    mom_block = jnp.concatenate(per_mom, axis=0)
    per_slab = [jnp.transpose(mom_block, (1, 0, 2, 3))]
    summed = lax.psum_scatter(jnp.stack(per_slab, axis=1), "space", scatter_dimension=0, tiled=True)
    dir_select = (directions[:, None] == jnp.arange(NDIR, dtype=jnp.int32)[None, :]).astype(
        jnp.float32
    )
    return jnp.einsum("dm,itpmq->itpdq", dir_select, summed, precision=lax.Precision.HIGHEST)


LANES = 128


def add_links(link, rows, field, sign):
    real, imag = [], []
    for a in range(3):
        re_sum = im_sum = None
        for b in range(3):
            row = rows + (3 * a + b if sign > 0 else 3 * b + a)
            link_re, link_im = link(row), link(row + 9)
            re_b, im_b = field[b], field[3 + b]
            if sign > 0:
                re_t = link_re * re_b - link_im * im_b
                im_t = link_re * im_b + link_im * re_b
            else:
                re_t = link_re * re_b + link_im * im_b
                im_t = link_re * im_b - link_im * re_b
            re_sum = re_t if re_sum is None else re_sum + re_t
            im_sum = im_t if im_sum is None else im_sum + im_t
        real.append(re_sum)
        imag.append(im_sum)
    return real + imag


def spread(tiles, lane_group, roll):
    first = []
    for a, b in ((0, 1), (2, 3)):
        even = lane_group % 2 == 0
        first.append(jnp.where(even, tiles[a], roll(tiles[b], LXY)))
        first.append(jnp.where(even, roll(tiles[a], -LXY), tiles[b]))
    low = lane_group < 2
    out = [None] * 4
    for bit in range(2):
        near, far = first[bit], first[2 + bit]
        out[bit] = jnp.where(low, near, roll(far, 2 * LXY))
        out[2 + bit] = jnp.where(low, roll(near, -2 * LXY), far)
    return out


def kernel(
    count, depth, groups, field_ref, links_ref, momenta_ref, directions_ref, out_ref,
    local, stage, held, halo, held_links, wide_links, tab_ref, twisted, packed, packed_y, acc, acc_y, sent, got, sent_y, got_y, sums,
    pay_send, pay_recv, halo_send, halo_recv, pass_send, pass_recv, link_send, link_recv, own_sem, part_send, part_recv,
):
    me = lax.axis_index("space")
    peers = lambda step: lax.rem(me + step, count)
    rows_of = field_ref.shape[3]
    eigs = count * rows_of
    moms = momenta_ref.shape[1]
    per_row = LANES // LXY
    pieces = depth // per_row
    row_k = 6 * pieces * LANES
    tall = count // 2
    half = lax.rem(me, 2)
    high = me // 2
    place_of = lambda device: lax.rem(device, 2) * (count - 1 - 2 * (device // 2)) + device // 2
    block = place_of(me)
    crossings = (tall // 2 - 1, tall + tall // 2 - 1)
    device_at = lambda place: 2 * place if place < tall else 2 * (count - 1 - place) + 1
    remote = lambda **rest: pltpu.make_async_remote_copy(device_id_type=pl.DeviceIdType.MESH, **rest)

    own_field = pltpu.make_async_copy(field_ref, local, own_sem.at[0])
    own_field.start()
    barrier = pltpu.get_barrier_semaphore()
    for step in range(1, count):
        pl.semaphore_signal(barrier, inc=1, device_id={"space": peers(step)}, device_id_type=pl.DeviceIdType.MESH)
    own_links = pltpu.make_async_copy(
        links_ref.at[:, :, pl.ds(pl.multiple_of(block * LANES, LANES), LANES)], held_links.at[me], own_sem.at[1]
    )
    own_links.start()

    def link_copy(target, source):
        return remote(
            src_ref=links_ref.at[:, :, pl.ds(pl.multiple_of(place_of(target) * LANES, LANES), LANES)],
            dst_ref=held_links.at[source],
            send_sem=link_send.at[target], recv_sem=link_recv.at[source], device_id={"space": target},
        )

    def pay_copy(row, target, source):
        return remote(
            src_ref=stage.at[place_of(target), row], dst_ref=held.at[row, source],
            send_sem=pay_send.at[row, target], recv_sem=pay_recv.at[row, source], device_id={"space": target},
        )

    def halo_copy(cross, source):
        place = crossings[cross]
        return remote(
            src_ref=stage.at[(place + 1) % count, 0], dst_ref=halo.at[source],
            send_sem=halo_send.at[cross], recv_sem=halo_recv.at[source], device_id={"space": device_at(place)},
        )

    def pass_copy():
        behind = lax.rem(block + count - 1, count)
        back = jnp.where(behind < tall, 2 * behind, 2 * (count - 1 - behind) + 1)
        return remote(
            src_ref=held.at[0], dst_ref=halo, send_sem=pass_send.at[0], recv_sem=pass_recv.at[0],
            device_id={"space": back},
        )

    def part_copy(group, target, source):
        return remote(
            src_ref=(sent, sent_y)[group].at[target], dst_ref=(got, got_y)[group].at[source],
            send_sem=part_send.at[group, target], recv_sem=part_recv.at[group, source], device_id={"space": target},
        )

    at_crossing = (block == crossings[0]) | (block == crossings[1])
    after_crossing = (block == crossings[0] + 1) | (block == (crossings[1] + 1) % count)
    roll = lambda value, shift: pltpu.roll(value, shift % LANES, 1)
    group_of = lambda rows: lax.broadcasted_iota(jnp.int32, (rows, LANES), 1) // LXY
    own_field.wait()

    def arrange(target, carry):
        lanes = group_of(rows_of)
        for c in range(6):
            for m in range(pieces):
                tiles = [local[c, m * per_row + q, target].astype(jnp.float32) for q in range(per_row)]
                for r, tile in enumerate(spread(tiles, lanes, roll)):
                    stage[target, r, c, m] = tile.astype(jnp.bfloat16)
        return carry

    lax.fori_loop(0, count, arrange, 0)
    pl.semaphore_wait(barrier, count - 1)

    for step in range(1, count):
        link_copy(peers(step), me).start()
    order = [0] + [d if s == 0 else tall - d for d in range(1, (tall + 1) // 2) for s in (0, 1)]
    if tall % 2 == 0:
        order.append(tall // 2)
    column = lambda hop: lax.rem(high + hop, tall)
    beside = [(hop, side) for hop in order for side in (1, 0)][:]
    beside.remove((0, 0))
    far = sorted(beside, key=lambda hop: -min(hop[0], tall - hop[0]))
    outer = (high == 0) | (high == tall - 1)

    def send_row(row):
        for hop, side in far:
            pay_copy(row, 2 * column(hop) + lax.rem(half + side, 2), me).start()

    send_row(0)
    send_row(1)
    for cross, place in enumerate(crossings):
        @pl.when(me != device_at(place))
        def _():
            halo_copy(cross, me).start()

    @pl.when(jnp.logical_not(outer))
    def _():
        for row in range(2, per_row):
            send_row(row)

    for row in range(per_row):
        held[row, me] = stage[block, row]

    @pl.when(at_crossing)
    def _():
        halo[me] = stage[lax.rem(block + 1, count), 0]

    mom_row = lax.broadcasted_iota(jnp.int32, (moms, LANES), 0)
    mom_lane = lax.broadcasted_iota(jnp.int32, (moms, LANES), 1)
    moved = []
    for axis in range(3):
        values = jnp.zeros((moms, LANES), jnp.int32)
        for p in range(moms):
            values = jnp.where(mom_row == p, momenta_ref[axis, p], values)
        moved.append(values)
    part_x = ((moved[0] * (mom_lane % LXY)) & (LXY - 1)).astype(jnp.float32) / LXY
    for row in range(per_row + 1):
        for m in range(pieces):
            y_at = block * per_row + row
            z_at = m * per_row + mom_lane // LXY
            fraction = part_x + ((moved[1] * y_at) & (LXY - 1)).astype(jnp.float32) / LXY
            fraction = fraction + ((moved[2] * z_at) & (depth - 1)).astype(jnp.float32) / depth
            tab_ref[row * pieces + m, 0:moms] = jnp.cos(TWO_PI * fraction)
            tab_ref[row * pieces + m, moms:] = jnp.sin(TWO_PI * fraction)

    own_links.wait()
    for step in range(1, count):
        link_copy(peers(step), peers(step)).wait_recv()
    for m in range(pieces):
        for mu in range(NDIR):
            tiles = [held_links[m * per_row + q, mu].astype(jnp.float32) for q in range(per_row)]
            for r, tile in enumerate(spread(tiles, group_of(tiles[0].shape[0]), roll)):
                wide_links[r, m, mu] = 0.5 * tile

    wide = 2 * rows_of
    x_of = lax.rem(lax.broadcasted_iota(jnp.int32, (wide, LANES), 1), LXY)
    quarter = group_of(wide)

    def next_x(value):
        return jnp.where(x_of == LXY - 1, roll(value, LXY - 1), roll(value, -1))

    def last_x(value):
        return jnp.where(x_of == 0, roll(value, 1 - LXY), roll(value, 1))

    def links_at(row, m):
        return lambda entry: wide_links[row, m, entry // 18, entry % 18][None]

    def load_from(ref, pair, row, m):
        if row is None:
            return [ref[pl.ds(2 * pair, 2), c, m].astype(jnp.float32).reshape(wide, LANES) for c in range(6)]
        return [ref[row, pl.ds(2 * pair, 2), c, m].astype(jnp.float32).reshape(wide, LANES) for c in range(6)]

    def store_packed(ref, base, first, values, row, m):
        vals = [value.astype(jnp.bfloat16) for value in values]
        for c in range(6):
            span = pl.ds(row * row_k + (c * pieces + m) * LANES, LANES)
            ref[pl.ds(base + first, wide), span] = vals[c]
            ref[pl.ds(base + eigs + first, wide), span] = vals[c + 3] if c < 3 else -vals[c - 3]

    def twist(field, first, row, m):
        for p in range(moms):
            cosine = tab_ref[row * pieces + m, p][None]
            sine = tab_ref[row * pieces + m, moms + p][None]
            for c in range(3):
                real = field[c] * cosine - field[c + 3] * sine
                imag = field[c] * sine + field[c + 3] * cosine
                for part, value in ((c, real), (c + 3, imag)):
                    span = pl.ds(row * row_k + (part * pieces + m) * LANES, LANES)
                    twisted[pl.ds(p * eigs + first, wide), span] = value.astype(jnp.bfloat16)

    def along_y(pair, first, row, m):
        ahead = load_from(held, pair, row + 1, m) if row + 1 < per_row else load_from(halo, pair, None, m)
        values = add_links(links_at(row, m), 18, ahead, 1)
        if row:
            behind = add_links(links_at(row - 1, m), 18, load_from(held, pair, row - 1, m), -1)
            values = [f - b for f, b in zip(values, behind)]
        store_packed(packed_y, 0, first, values, row, m)

    def do_row(row, pair):
        first = pl.multiple_of(pair * wide, wide)
        behind = []
        for m in range(pieces):
            field = load_from(held, pair, row, m)
            twist(field, first, row, m)
            forward = add_links(links_at(row, m), 0, [next_x(v) for v in field], 1)
            backward = [last_x(v) for v in add_links(links_at(row, m), 0, field, -1)]
            store_packed(packed, 0, first, [f - b for f, b in zip(forward, backward)], row, m)
        for m in range(pieces):
            behind.append([roll(v, LXY) for v in add_links(links_at(row, m), 36, load_from(held, pair, row, m), -1)])
        for m in range(pieces):
            field, after = load_from(held, pair, row, m), load_from(held, pair, row, (m + 1) % pieces)
            shifted = [
                jnp.where(quarter == per_row - 1, roll(a, -LXY), roll(v, -LXY)) for v, a in zip(field, after)
            ]
            forward = add_links(links_at(row, m), 36, shifted, 1)
            backward = [
                jnp.where(quarter == 0, a, b) for a, b in zip(behind[(m - 1) % pieces], behind[m])
            ]
            store_packed(packed, 2 * eigs, first, [f - b for f, b in zip(forward, backward)], row, m)
        if 0 < row < per_row - 1:
            for m in range(pieces):
                along_y(pair, first, row - 1, m)

    def finish_y(pair, carry):
        first = pl.multiple_of(pair * wide, wide)
        for m in range(pieces):
            along_y(pair, first, per_row - 2, m)
            along_y(pair, first, per_row - 1, m)
            tails = add_links(links_at(per_row - 1, m), 18, load_from(held, pair, per_row - 1, m), -1)
            store_packed(packed_y, 0, first, [-v for v in tails], per_row, m)
        return carry

    contract = (((1,), (1,)), ((), ()))

    def dot_of(rows, ref, first_row, last_row):
        span = slice(first_row * row_k, last_row * row_k)
        middle = (rows.start + rows.stop) // 2
        parts = [
            lax.dot_general(twisted[part, span], ref[:, span], contract, preferred_element_type=jnp.float32)
            for part in (slice(rows.start, middle), slice(middle, rows.stop))
        ]
        return jnp.concatenate(parts, axis=0)

    every = slice(0, moms * eigs)
    for row in range(per_row):
        def one(i, carry):
            pair = column(jnp.where(i < 2, i, tall + 1 - i))
            for side in range(2):
                source = 2 * pair + side

                @pl.when(source != me)
                def _():
                    pay_copy(row, source, source).wait_recv()
            do_row(row, pair)
            return carry

        lax.fori_loop(0, tall, one, 0)
        if row + 2 < per_row:
            @pl.when(outer)
            def _():
                send_row(row + 2)
        if row == 0:
            @pl.when(jnp.logical_not(after_crossing))
            def _():
                pass_copy().start()
            acc[...] = dot_of(every, packed, 0, 1)
        if row == 1:
            acc[...] += dot_of(every, packed, 1, 2)
            acc_y[...] = dot_of(every, packed_y, 0, 1)
        if row == 2:
            acc[...] += dot_of(every, packed, 2, 3)
        if row == 1:
            @pl.when(at_crossing)
            def _():
                for step in range(1, count):
                    halo_copy(0, peers(step)).wait_recv()

            @pl.when(jnp.logical_not(at_crossing))
            def _():
                pass_copy().wait_recv()

            def last(pair, carry):
                for m in range(pieces):
                    twist(load_from(halo, pair, None, m), pl.multiple_of(pair * wide, wide), per_row, m)
                return carry

            lax.fori_loop(0, tall, last, 0)

    width = 2 * eigs

    def scatter(group, result, index):
        result = result.reshape(moms, count, rows_of, width)
        for p in range(moms):
            for target in range(count):
                (sent, sent_y)[group][(target, p) + index] = result[p, target].astype(jnp.bfloat16)

    along = acc[...] + dot_of(every, packed, per_row - 1, per_row)
    for d in range(2):
        scatter(0, along[:, d * width : (d + 1) * width], (d,))
    reach = [2 * column(hop) + lax.rem(half + side, 2) for hop, side in far]
    for target in reach:
        part_copy(0, target, me).start()
    lax.fori_loop(0, tall, finish_y, 0)
    scatter(1, acc_y[...] + dot_of(every, packed_y, 1, per_row + 1), ())
    for target in reach:
        part_copy(1, target, me).start()

    got[me] = sent[me]
    got_y[me] = sent_y[me]
    for group in range(groups):
        for step in range(1, count):
            part_copy(group, peers(step), peers(step)).wait_recv()
        for p in range(moms):
            for d in range(2 - group):
                at = (p, d) if group == 0 else (p,)
                buffer = (got, got_y)[group]
                total = buffer[(0,) + at].astype(jnp.float32)
                for source in range(1, count):
                    total = total + buffer[(source,) + at].astype(jnp.float32)
                sums[2 * d if group == 0 else 1, p] = total
    for d in range(NDIR):
        for p in range(moms):
            out_ref[:, d, p] = sums[directions_ref[d], p]

    for step in range(1, count):
        target = peers(step)
        link_copy(target, me).wait_send()
        for row in range(per_row):
            pay_copy(row, target, me).wait_send()
        for group in range(groups):
            part_copy(group, target, me).wait_send()
    for cross, place in enumerate(crossings):
        @pl.when(me != device_at(place))
        def _():
            halo_copy(cross, me).wait_send()

    @pl.when(jnp.logical_not(after_crossing))
    def _():
        pass_copy().wait_send()


def shards_by_rows(vectors, gauge_links, momenta, directions):
    count = lax.axis_size("space")
    eig_local = vectors.shape[1]
    eigs = eig_local * count
    moms = momenta.shape[0]
    depth = vectors.shape[3] // (LXY * LXY)
    per_row = LANES // LXY
    pieces = depth // per_row
    field = jnp.transpose(vectors[0].reshape(eig_local, 6, depth, count, LANES), (1, 2, 3, 0, 4))

    groups = 2
    row_k = 6 * pieces * LANES
    vmem = pl.BlockSpec(memory_space=pltpu.VMEM)
    part = (count, moms, 2, eig_local, 2 * eigs)
    part_y = (count, moms, eig_local, 2 * eigs)
    lump = (6, pieces, eig_local, LANES)
    summed = pl.pallas_call(
        lambda *refs: kernel(count, depth, groups, *refs),
        out_shape=jax.ShapeDtypeStruct((eig_local, NDIR, moms, 2 * eigs), jnp.float32),
        in_specs=[
            pl.BlockSpec(memory_space=pl.ANY),
            pl.BlockSpec(memory_space=pl.ANY),
            pl.BlockSpec(memory_space=pltpu.SMEM),
            pl.BlockSpec(memory_space=pltpu.SMEM),
        ],
        out_specs=vmem,
        scratch_shapes=[
            pltpu.VMEM(field.shape, jnp.bfloat16),
            pltpu.VMEM((count, per_row) + lump, jnp.bfloat16),
            pltpu.VMEM((per_row, count) + lump, jnp.bfloat16),
            pltpu.VMEM((count,) + lump, jnp.bfloat16),
            pltpu.VMEM((count, NDIR, 18, LANES), jnp.bfloat16),
            pltpu.VMEM((per_row, pieces, NDIR, 18, LANES), jnp.float32),
            pltpu.VMEM(((per_row + 1) * pieces, 2 * moms, LANES), jnp.float32),
            pltpu.VMEM((moms * eigs, (per_row + 1) * row_k), jnp.bfloat16),
            pltpu.VMEM((4 * eigs, per_row * row_k), jnp.bfloat16),
            pltpu.VMEM((2 * eigs, (per_row + 1) * row_k), jnp.bfloat16),
            pltpu.VMEM((moms * eigs, 4 * eigs), jnp.float32),
            pltpu.VMEM((moms * eigs, 2 * eigs), jnp.float32),
            pltpu.VMEM(part, jnp.bfloat16),
            pltpu.VMEM(part, jnp.bfloat16),
            pltpu.VMEM(part_y, jnp.bfloat16),
            pltpu.VMEM(part_y, jnp.bfloat16),
            pltpu.VMEM((NDIR, moms, eig_local, 2 * eigs), jnp.float32),
            pltpu.SemaphoreType.DMA((per_row, count)),
            pltpu.SemaphoreType.DMA((per_row, count)),
            pltpu.SemaphoreType.DMA((2,)),
            pltpu.SemaphoreType.DMA((count,)),
            pltpu.SemaphoreType.DMA((1,)),
            pltpu.SemaphoreType.DMA((1,)),
            pltpu.SemaphoreType.DMA((count,)),
            pltpu.SemaphoreType.DMA((count,)),
            pltpu.SemaphoreType.DMA((2,)),
            pltpu.SemaphoreType.DMA((groups, count)),
            pltpu.SemaphoreType.DMA((groups, count)),
        ],
        compiler_params=pltpu.CompilerParams(collective_id=0, has_side_effects=True, vmem_limit_bytes=55700000),
        name="elementals",
    )(field, gauge_links[0], momenta.T, directions)
    return jnp.transpose(summed, (0, 2, 1, 3))[:, None]


def shards(vectors, gauge_links, momenta, directions):
    count = lax.axis_size("space")
    depth = vectors.shape[3] // (LXY * LXY)
    by_rows = (
        vectors.shape[0] == 1
        and count * LANES == LXY * LXY
        and depth == count
        and depth & (depth - 1) == 0
        and depth == 2 * (LANES // LXY)
        and vectors.shape[1] % 8 == 0
    )
    body = shards_by_rows if by_rows else shards_by_plane
    return body(vectors, gauge_links, momenta, directions)


def solution(mesh):
    return jax.shard_map(
        shards,
        mesh=mesh,
        in_specs=(
            P(("cfg", "tm"), "space", None, None),
            P(("cfg", "tm"), None, None, "space"),
            P(),
            P(),
        ),
        out_specs=P("space", ("cfg", "tm"), None, None, None),
        check_vma=False,
    )
```
